32 devices in a mesh: row: 2 (over x), col: 16 (over z, y, core).
Axes of the slice: x: 2, y: 2, z: 4, core: 2. Of those that a mesh axis runs over, the one named last changes fastest.
Arguments:
- tokens: bfloat16 [64, 128, 1024], P('row', 'col'), may hold values from -6 to 6
- shifts: int32 [2], replicated, may hold values from 0 to 15
- qkv_weight: bfloat16 [1024, 3, 1024], P('col', None, 'row'), may hold values from -0.1875 to 0.1875
- out_weight: bfloat16 [1024, 1024], P('row', 'col'), may hold values from -0.1875 to 0.1875
- up_weight: bfloat16 [1024, 4096], P('col', 'row'), may hold values from -0.1875 to 0.1875
- down_weight: bfloat16 [4096, 1024], P('row', 'col'), may hold values from -0.09375 to 0.09375
- qk_gain: float32 [1024], P('row'), may hold values from 0.5 to 1.5
- attn_rate: float32 [1024], replicated, may hold values from 0.1 to 0.6
- mlp_rate: float32 [1024], replicated, may hold values from 0.1 to 0.6
- hidden_gain: float32 [4096], P('row'), may hold values from 0.5 to 2
Outputs:
- sphere_out: bfloat16 [64, 128, 1024], P('row', 'col')
The draws below stay inside these ranges and needn't reach their ends.
Inputs may be any that keep to these rules, and one draw needn't show every extreme that they name: shifts[0] offsets the windows along rows, shifts[1] along columns.
All inputs are finite; a program needn't handle non-finite values.
Results may differ from the reference program's by a relative error of at most 0.012.
Values may be sent and summed in bfloat16 or wider, within the bound.
A program may use at most 128 MiB of HBM per device.

```python
import math
import jax
import jax.numpy as jnp
from jax import lax

D = 1024
H = 16
FF = 4096
HD = 64
WIN = 16
GRID_ROWS = 64
GRID_COLS = 128
N_ROW = 2


def levels(own_key, shape, shards, low, largest):
    def one(axis_at, parts):
        heights = jax.random.uniform(jax.random.fold_in(jax.random.fold_in(own_key, 6), axis_at), (parts,), jnp.float32, low / len(shards), largest / len(shards))
        return jnp.repeat(jnp.exp(heights), shape[axis_at] // parts).reshape((-1,) + (1,) * (len(shape) - axis_at - 1))

    loudness = one(*shards[0])
    for cut in shards[1:]:
        loudness = loudness * one(*cut)
    return loudness


def bell_draw(own_key, dims, scale, limit, shards=(), kind=jnp.bfloat16):
    drawn = scale * jax.random.normal(own_key, dims, jnp.float32)
    if shards:
        drawn = drawn * levels(own_key, dims, shards, -0.22, 0.18)
    return jnp.clip(drawn, -limit, limit).astype(kind)


def setup_inputs(seed: int = 0) -> dict:
    streams_of = jax.random.split(jax.random.key(seed), 11)
    return {
        "tokens": bell_draw(streams_of[0], (GRID_ROWS, GRID_COLS, D), 1.0, 6.0, ((0, 2), (1, 16))),
        "shifts": jax.random.randint(streams_of[1], (2,), 0, WIN).astype(jnp.int32),
        "qkv_weight": bell_draw(streams_of[2], (D, 3, D), D ** -0.5, 0.1875, ((0, 16), (2, 2))),
        "out_weight": bell_draw(streams_of[3], (D, D), D ** -0.5, 0.1875, ((0, 2), (1, 16))),
        "up_weight": bell_draw(streams_of[4], (D, FF), D ** -0.5, 0.1875, ((0, 16), (1, 2))),
        "down_weight": bell_draw(streams_of[5], (FF, D), FF ** -0.5, 0.09375, ((0, 2), (1, 16))),
        "qk_gain": jnp.clip(jnp.exp(math.log(1.5) - 1.0986123 * jax.random.uniform(streams_of[6], (D,), jnp.float32) ** levels(streams_of[6], (D,), ((0, 2),), -0.2, 0.2)), 0.5, 1.5),
        "attn_rate": jnp.clip(jnp.exp(jax.random.uniform(streams_of[7], (D,), jnp.float32, math.log(0.1), math.log(0.6))), 0.1, 0.6),
        "mlp_rate": jnp.clip(jnp.exp(jax.random.uniform(streams_of[8], (D,), jnp.float32, math.log(0.1), math.log(0.6))), 0.1, 0.6),
        "hidden_gain": jnp.clip(jnp.exp(math.log(2.0) - 1.3862944 * jax.random.uniform(streams_of[9], (FF,), jnp.float32) ** levels(streams_of[9], (FF,), ((0, 2),), -0.2, 0.2)), 0.5, 2.0),
    }


def to_sphere(vector):
    return vector * lax.rsqrt(lax.optimization_barrier(jnp.mean(vector * vector, axis=-1, keepdims=True)) + 1e-06)

def rounded(vector):
    return lax.optimization_barrier(vector.astype(jnp.bfloat16)).astype(jnp.float32)

def window_band(operands):
    query_band, key_band, value_band = operands
    scores = jnp.einsum('wqhd,wkhd->whqk', query_band.astype(jnp.float32), key_band.astype(jnp.float32)) / math.sqrt(HD)
    expo = jnp.exp(scores)
    weights = (expo / lax.optimization_barrier(jnp.sum(expo, axis=-1, keepdims=True))).astype(jnp.bfloat16)
    return jnp.einsum('whqk,wkhd->wqhd', weights.astype(jnp.float32), value_band.astype(jnp.float32)).astype(jnp.bfloat16)

def reference(tokens, shifts, qkv_weight, out_weight, up_weight, down_weight, qk_gain, attn_rate, mlp_rate, hidden_gain):
    grid_rows = tokens.shape[0]
    grid_cols = tokens.shape[1]
    token_count = grid_rows * grid_cols
    sphere = to_sphere(tokens.astype(jnp.float32)).reshape(token_count, D)
    sphere_bf = sphere.astype(jnp.bfloat16)
    projected = jnp.dot(sphere_bf, qkv_weight.reshape(D, 3 * D), preferred_element_type=jnp.float32)
    projected = projected.reshape(grid_rows, grid_cols, 3, H, HD)
    head_gain = qk_gain.reshape(H, HD)
    queries = (to_sphere(projected[:, :, 0]) * head_gain).astype(jnp.bfloat16)
    keys_sphere = (to_sphere(projected[:, :, 1]) * head_gain).astype(jnp.bfloat16)
    values = projected[:, :, 2].astype(jnp.bfloat16)
    shift_row = shifts[0]
    shift_col = shifts[1]

    def to_windows(field):
        rolled = jnp.roll(jnp.roll(field, -shift_row, axis=0), -shift_col, axis=1)
        rolled = rolled.reshape(grid_rows // WIN, WIN, grid_cols // WIN, WIN, H, HD)
        return rolled.transpose(0, 2, 1, 3, 4, 5).reshape(grid_rows // WIN, grid_cols // WIN, WIN * WIN, H, HD)
    attended = lax.map(window_band, (to_windows(queries), to_windows(keys_sphere), to_windows(values)))
    attended = attended.reshape(grid_rows // WIN, grid_cols // WIN, WIN, WIN, H, HD)
    attended = attended.transpose(0, 2, 1, 3, 4, 5).reshape(grid_rows, grid_cols, D)
    attended = jnp.roll(jnp.roll(attended, shift_row, axis=0), shift_col, axis=1).reshape(token_count, D)
    group_width = D // N_ROW
    attn_total = jnp.zeros((token_count, D), jnp.float32)
    for group_index in range(N_ROW):
        first = group_index * group_width
        attn_total = attn_total + rounded(jnp.dot(attended[:, first:first + group_width], out_weight[first:first + group_width], preferred_element_type=jnp.float32))
    mixed = to_sphere(sphere + attn_rate * (to_sphere(attn_total) - sphere))
    mixed_bf = mixed.astype(jnp.bfloat16)
    hidden_width = FF // N_ROW
    mlp_total = jnp.zeros((token_count, D), jnp.float32)
    for group_index in range(N_ROW):
        first = group_index * hidden_width
        raised = jnp.dot(mixed_bf, up_weight[:, first:first + hidden_width], preferred_element_type=jnp.float32) * hidden_gain[first:first + hidden_width]
        activated = jax.nn.gelu(raised, approximate=False).astype(jnp.bfloat16)
        mlp_total = mlp_total + rounded(jnp.dot(activated, down_weight[first:first + hidden_width], preferred_element_type=jnp.float32))
    sphere_out = to_sphere(mixed + mlp_rate * (to_sphere(mlp_total) - mixed))
    return sphere_out.astype(jnp.bfloat16).reshape(grid_rows, grid_cols, D)
```

```python
import functools
import math

import jax
import jax.numpy as jnp
from jax import lax
from jax.experimental import pallas as pl
from jax.experimental.pallas import tpu as pltpu
from jax.sharding import PartitionSpec as P

HD = 64
WIN = 16
MESH = pl.DeviceIdType.MESH
VMEM = pl.BlockSpec(memory_space=pltpu.VMEM)


def shifted(value, axis, steps):
    count = lax.axis_size(axis)
    pairs = [(source, (source + steps) % count) for source in range(count)]
    return lax.ppermute(value, axis, pairs)


def to_sphere(vector):
    return vector * lax.rsqrt(jnp.mean(vector * vector, axis=-1, keepdims=True) + 1e-06)


def gather_kernel(n_row, n_col, reach, n_weights, *refs):
    tok_in = refs[0]
    w_in = refs[1 : 1 + n_weights]
    tok_out = refs[1 + n_weights]
    w_out = refs[2 + n_weights : 2 + 2 * n_weights]
    send_sem, recv_sem = refs[2 + 2 * n_weights :]
    row = lax.axis_index("row")
    col = lax.axis_index("col")
    nz = n_col // 4
    z = col // 4
    y = (col // 2) % 2
    core = col % 2

    def at(zz, yy, cc):
        return (lax.rem(zz + 2 * nz, nz) * 2 + yy) * 2 + cc

    z_next = at(z + 1, y, core)
    z_prev = at(z - 1, y, core)
    y_peer = at(z, 1 - y, core)
    core_peer = at(z, y, 1 - core)
    greet = [(row, z_next), (row, z_prev), (row, y_peer), (row, core_peer)]
    for k in range(1, reach + 1):
        greet.append((row, lax.rem(col + k, n_col)))
        greet.append((row, lax.rem(col - k + n_col, n_col)))
    for r in range(1, n_row):
        greet.append((lax.rem(row + r, n_row), col))
    barrier = pltpu.get_barrier_semaphore()
    for peer in greet:
        pl.semaphore_signal(barrier, inc=1, device_id=peer, device_id_type=MESH)
    pl.semaphore_wait(barrier, len(greet))

    started = []

    def send(src, dst, peer):
        index = len(started)
        copy = pltpu.make_async_remote_copy(
            src_ref=src,
            dst_ref=dst,
            send_sem=send_sem.at[index],
            recv_sem=recv_sem.at[index],
            device_id=peer,
            device_id_type=MESH,
        )
        copy.start()
        started.append(copy)
        return copy

    near = {}
    far = []
    for r in range(1, n_row):
        far.append(send(tok_in, tok_out.at[row, 0], (lax.rem(row + r, n_row), col)))
    for k in range(1, reach + 1):
        near[k] = send(tok_in, tok_out.at[row, k], (row, lax.rem(col - k + n_col, n_col)))
    z_copy, y_copy, core_copies = {}, {}, []
    for w in range(n_weights):
        z_copy[w, 0] = send(w_in[w], w_out[w].at[col], (row, z_next))
        y_copy[w, 0] = send(w_in[w], w_out[w].at[col], (row, y_peer))
        core_copies.append(send(w_in[w], w_out[w].at[col], (row, core_peer)))
    tok_out[row, 0] = tok_in[...]
    for w in range(n_weights):
        w_out[w][col] = w_in[w][...]
    for t in range(nz):
        for w in range(n_weights):
            if t > 0:
                z_copy[w, t - 1].wait_recv()
                block = w_out[w].at[at(z - t, y, core)]
                if t < nz - 1:
                    z_copy[w, t] = send(block, block, (row, z_next))
                y_copy[w, t] = send(block, block, (row, y_peer))
                core_copies.append(send(block, block, (row, core_peer)))
            y_copy[w, t].wait_recv()
            other = w_out[w].at[at(z - t, 1 - y, core)]
            core_copies.append(send(other, other, (row, core_peer)))
        if t == 0:
            for k in range(1, reach + 1):
                near[k].wait_recv()
                piece = tok_out.at[row, k]
                for r in range(1, n_row):
                    far.append(send(piece, piece, (lax.rem(row + r, n_row), col)))
    for copy in far:
        copy.wait_recv()
    for copy in core_copies:
        copy.wait_recv()
    for copy in started:
        copy.wait_send()


def gather_all(tokens, weights, n_row, n_col, reach):
    nz = n_col // 4
    n_weights = len(weights)
    copies = reach * n_row + (n_row - 1) + n_weights * (nz - 1 + nz + 2 * nz)
    return pl.pallas_call(
        functools.partial(gather_kernel, n_row, n_col, reach, n_weights),
        out_shape=[jax.ShapeDtypeStruct((n_row, reach + 1) + tokens.shape, tokens.dtype)]
        + [jax.ShapeDtypeStruct((n_col,) + w.shape, w.dtype) for w in weights],
        in_specs=[VMEM] * (1 + n_weights),
        out_specs=[VMEM] * (1 + n_weights),
        scratch_shapes=[pltpu.SemaphoreType.DMA((copies,)), pltpu.SemaphoreType.DMA((copies,))],
        compiler_params=pltpu.CompilerParams(
            collective_id=0, has_side_effects=True, vmem_limit_bytes=48 * 1024 * 1024
        ),
        name="gather_all",
    )(tokens, *weights)


def project_kernel(heads, x_ref, w_ref, gain_ref, q_ref, kv_ref):
    width = heads * HD
    projected = jnp.dot(x_ref[...], w_ref[...], preferred_element_type=jnp.float32)
    for part in range(2):
        for head in range(heads):
            lo = head * HD
            piece = projected[:, part * width + lo : part * width + lo + HD]
            scaled = (to_sphere(piece) * gain_ref[:, lo : lo + HD]).astype(jnp.bfloat16)
            if part == 0:
                q_ref[:, lo : lo + HD] = scaled
            else:
                kv_ref[0, :, lo : lo + HD] = scaled
    kv_ref[1] = projected[:, 2 * width :].astype(jnp.bfloat16)


def project(x, weight, gain, heads):
    tokens, depth = x.shape
    width = heads * HD
    block = math.gcd(tokens, 128)
    return pl.pallas_call(
        functools.partial(project_kernel, heads),
        grid=(tokens // block,),
        out_shape=[
            jax.ShapeDtypeStruct((tokens, width), jnp.bfloat16),
            jax.ShapeDtypeStruct((2, tokens, width), jnp.bfloat16),
        ],
        in_specs=[
            pl.BlockSpec((block, depth), lambda i: (i, 0)),
            pl.BlockSpec((depth, 3 * width), lambda i: (0, 0)),
            pl.BlockSpec((1, width), lambda i: (0, 0)),
        ],
        out_specs=[
            pl.BlockSpec((block, width), lambda i: (i, 0)),
            pl.BlockSpec((2, block, width), lambda i: (0, i, 0)),
        ],
        name="project",
        cost_estimate=pl.CostEstimate(
            flops=6 * tokens * depth * width, bytes_accessed=8 * depth * width, transcendentals=0
        ),
    )(x, weight, gain.reshape(1, width))


def attend_kernel(heads, q_ref, *refs):
    out_ref = refs[-1]
    kv_refs = refs[:-1]
    contract = (((1,), (1,)), ((), ()))
    for head in range(heads):
        cut = slice(head * HD, head * HD + HD)
        query = q_ref[:, cut]
        keys = jnp.concatenate([kv[0, :, cut] for kv in kv_refs], axis=0)
        values = jnp.concatenate([kv[1, :, cut] for kv in kv_refs], axis=0)
        scores = lax.dot_general(query, keys, contract, preferred_element_type=jnp.float32)
        expo = jnp.exp(scores * (1.0 / math.sqrt(HD)))
        weights = (expo / jnp.sum(expo, axis=-1, keepdims=True)).astype(jnp.bfloat16)
        out_ref[:, cut] = jnp.dot(weights, values, preferred_element_type=jnp.float32).astype(
            jnp.bfloat16
        )


def attend(queries, kv_parts, heads, band):
    tokens, width = queries.shape
    return pl.pallas_call(
        functools.partial(attend_kernel, heads),
        grid=(tokens // band,),
        out_shape=jax.ShapeDtypeStruct((tokens, width), jnp.bfloat16),
        in_specs=[pl.BlockSpec((band, width), lambda i: (i, 0))]
        + [pl.BlockSpec((2, band, width), lambda i: (0, i, 0)) for _ in kv_parts],
        out_specs=pl.BlockSpec((band, width), lambda i: (i, 0)),
        name="attend",
        cost_estimate=pl.CostEstimate(
            flops=4 * tokens * band * width * len(kv_parts),
            bytes_accessed=6 * tokens * width,
            transcendentals=tokens * band * heads * len(kv_parts),
        ),
    )(queries, *kv_parts)


def on_device(
    tokens,
    shifts,
    qkv_weight,
    out_weight,
    up_weight,
    down_weight,
    qk_gain,
    attn_rate,
    mlp_rate,
    hidden_gain,
):
    n_row = lax.axis_size("row")
    n_col = lax.axis_size("col")
    row = lax.axis_index("row")
    local_rows, cols, width = tokens.shape
    local_width = qkv_weight.shape[2]
    hidden = up_weight.shape[1]
    heads = local_width // HD
    per_window = WIN // cols
    reach = (WIN + cols - 2) // cols
    strip_rows = local_rows * n_row
    count = strip_rows * cols
    shift_row, shift_col = shifts[0], shifts[1]

    gathered = gather_all(
        tokens.reshape(local_rows * cols, width),
        [
            qkv_weight.reshape(-1, 3 * local_width),
            out_weight.T,
            up_weight,
            down_weight.T,
        ],
        n_row,
        n_col,
        reach,
    )
    pieces = gathered[0].reshape(n_row, reach + 1, local_rows, cols, width)
    qkv_full = gathered[1].reshape(width, 3 * local_width)
    out_full = gathered[2].reshape(width, local_width)
    up_full = gathered[3].reshape(width, hidden)
    down_full = gathered[4].reshape(width, hidden)

    wide = pieces.transpose(0, 2, 1, 3, 4).reshape(strip_rows, (reach + 1) * cols, width)
    strip = lax.dynamic_slice_in_dim(wide, shift_col, cols, axis=1)
    normed = to_sphere(strip.astype(jnp.float32))
    flat = normed.reshape(count, width)
    rolled = jnp.roll(normed.astype(jnp.bfloat16), -shift_row, axis=0).reshape(count, width)
    queries, kv = project(rolled, qkv_full, qk_gain, heads)
    kv_parts = [kv]
    for k in range(1, per_window):
        pairs = [
            (c, c // per_window * per_window + (c + k) % per_window) for c in range(n_col)
        ]
        kv_parts.append(lax.ppermute(kv, "col", pairs))
    attended = attend(queries, kv_parts, heads, WIN * cols)
    attended = jnp.roll(
        attended.reshape(strip_rows, cols, local_width), shift_row, axis=0
    ).reshape(count, local_width)
    contract = (((1,), (1,)), ((), ()))
    attn_own = lax.dot_general(
        attended, out_full, contract, preferred_element_type=jnp.float32
    ).astype(jnp.bfloat16)
    attn_all = attn_own.astype(jnp.float32)
    for r in range(1, n_row):
        attn_all = attn_all + shifted(attn_own, "row", r).astype(jnp.float32)
    mixed = to_sphere(flat + attn_rate * (to_sphere(attn_all) - flat))
    raised = jnp.dot(mixed.astype(jnp.bfloat16), up_full, preferred_element_type=jnp.float32)
    activated = jax.nn.gelu(raised * hidden_gain, approximate=False).astype(jnp.bfloat16)
    mlp_own = lax.dot_general(
        activated, down_full, contract, preferred_element_type=jnp.float32
    ).astype(jnp.bfloat16)
    local = local_rows * cols

    def part(value, owner):
        return lax.dynamic_slice_in_dim(value, owner * local, local, 0)

    mlp_local = part(mlp_own, row).astype(jnp.float32)
    for r in range(1, n_row):
        there = part(mlp_own, lax.rem(row + r, n_row))
        mlp_local = mlp_local + shifted(there, "row", r).astype(jnp.float32)
    mixed_local = part(mixed, row)
    result = to_sphere(mixed_local + mlp_rate * (to_sphere(mlp_local) - mixed_local))
    result = result.astype(jnp.bfloat16).reshape(local_rows, cols, width)
    spread = [shifted(result, "col", k) for k in range(reach, 0, -1)] + [result]
    spread = jnp.concatenate(spread, axis=1)
    return lax.dynamic_slice_in_dim(spread, reach * cols - shift_col, cols, axis=1)


def solution(mesh):
    return jax.shard_map(
        on_device,
        mesh=mesh,
        in_specs=(
            P("row", "col", None),
            P(),
            P("col", None, "row"),
            P("row", "col"),
            P("col", "row"),
            P("row", "col"),
            P("row"),
            P(),
            P(),
            P("row"),
        ),
        out_specs=P("row", "col", None),
        check_vma=False,
    )
```

```python
import functools
import math

import jax
import jax.numpy as jnp
from jax import lax
from jax.experimental import pallas as pl
from jax.experimental.pallas import tpu as pltpu
from jax.sharding import PartitionSpec as P

HD = 64
WIN = 16
MESH = pl.DeviceIdType.MESH
VMEM = pl.BlockSpec(memory_space=pltpu.VMEM)


def shifted(value, axis, steps):
    count = lax.axis_size(axis)
    pairs = [(source, (source + steps) % count) for source in range(count)]
    return lax.ppermute(value, axis, pairs)


def to_sphere(vector):
    return vector * lax.rsqrt(jnp.mean(vector * vector, axis=-1, keepdims=True) + 1e-06)


class Ring:
    def __init__(self, n_row, n_col, send_sem, recv_sem):
        self.n_row, self.n_col, self.nz = n_row, n_col, n_col // 4
        self.send_sem, self.recv_sem = send_sem, recv_sem
        self.row, self.col = lax.axis_index("row"), lax.axis_index("col")
        self.z, self.y, self.core = self.col // 4, (self.col // 2) % 2, self.col % 2
        self.z_next = (self.row, self.at(self.z + 1, self.y, self.core))
        self.z_prev = (self.row, self.at(self.z - 1, self.y, self.core))
        self.y_peer = (self.row, self.at(self.z, 1 - self.y, self.core))
        self.core_peer = (self.row, self.at(self.z, self.y, 1 - self.core))
        self.started, self.core_copies, self.z_copy, self.y_copy = [], [], {}, {}

    def at(self, z, y, core):
        return (lax.rem(z + 2 * self.nz, self.nz) * 2 + y) * 2 + core

    def other_row(self, r):
        return (lax.rem(self.row + r, self.n_row), self.col)

    def greet(self, more):
        peers = [self.z_next, self.z_prev, self.y_peer, self.core_peer] + more
        peers += [self.other_row(r) for r in range(1, self.n_row)]
        barrier = pltpu.get_barrier_semaphore()
        for peer in peers:
            pl.semaphore_signal(barrier, inc=1, device_id=peer, device_id_type=MESH)
        pl.semaphore_wait(barrier, len(peers))

    def send(self, src, dst, peer):
        index = len(self.started)
        copy = pltpu.make_async_remote_copy(
            src_ref=src,
            dst_ref=dst,
            send_sem=self.send_sem.at[index],
            recv_sem=self.recv_sem.at[index],
            device_id=peer,
            device_id_type=MESH,
        )
        copy.start()
        self.started.append(copy)
        return copy

    def begin(self, w_in, w_out):
        for w in range(len(w_in)):
            slot = w_out[w].at[self.col]
            self.z_copy[w, 0] = self.send(w_in[w], slot, self.z_next)
            self.y_copy[w, 0] = self.send(w_in[w], slot, self.y_peer)
            self.core_copies.append(self.send(w_in[w], slot, self.core_peer))
        for w in range(len(w_in)):
            w_out[w][self.col] = w_in[w][...]

    def advance(self, t, w_out):
        for w in range(len(w_out)):
            if t > 0:
                self.z_copy[w, t - 1].wait_recv()
                block = w_out[w].at[self.at(self.z - t, self.y, self.core)]
                if t < self.nz - 1:
                    self.z_copy[w, t] = self.send(block, block, self.z_next)
                self.y_copy[w, t] = self.send(block, block, self.y_peer)
                self.core_copies.append(self.send(block, block, self.core_peer))
        for w in range(len(w_out)):
            self.y_copy[w, t].wait_recv()
            other = w_out[w].at[self.at(self.z - t, 1 - self.y, self.core)]
            self.core_copies.append(self.send(other, other, self.core_peer))

    def finish(self):
        for copy in self.core_copies:
            copy.wait_recv()
        for copy in self.started:
            copy.wait_send()


def gather_kernel(n_row, n_col, reach, n_weights, *refs):
    tok_in = refs[0]
    w_in = refs[1 : 1 + n_weights]
    tok_out = refs[1 + n_weights]
    w_out = refs[2 + n_weights : 2 + 2 * n_weights]
    ring = Ring(n_row, n_col, *refs[2 + 2 * n_weights :])
    row, col = ring.row, ring.col
    ring.greet(
        [(row, lax.rem(col + k, n_col)) for k in range(1, reach + 1)]
        + [(row, lax.rem(col - k + n_col, n_col)) for k in range(1, reach + 1)]
    )
    near = {}
    far = []
    for k in range(1, reach + 1):
        near[k] = ring.send(tok_in, tok_out.at[row, k], (row, lax.rem(col - k + n_col, n_col)))
    for r in range(1, n_row):
        far.append(ring.send(tok_in, tok_out.at[row, 0], ring.other_row(r)))
    ring.begin(w_in, w_out)
    tok_out[row, 0] = tok_in[...]
    for t in range(ring.nz):
        if t == 1:
            for k in range(1, reach + 1):
                near[k].wait_recv()
                piece = tok_out.at[row, k]
                for r in range(1, n_row):
                    far.append(ring.send(piece, piece, ring.other_row(r)))
        ring.advance(t, w_out)
    for copy in far:
        copy.wait_recv()
    ring.finish()


def ring_copies(n_col, n_weights):
    nz = n_col // 4
    return n_weights * (nz - 1 + nz + 2 * nz)


def gather_all(tokens, weights, n_row, n_col, reach):
    n_weights = len(weights)
    copies = reach * n_row + (n_row - 1) + ring_copies(n_col, n_weights)
    return pl.pallas_call(
        functools.partial(gather_kernel, n_row, n_col, reach, n_weights),
        out_shape=[jax.ShapeDtypeStruct((n_row, reach + 1) + tokens.shape, tokens.dtype)]
        + [jax.ShapeDtypeStruct((n_col,) + w.shape, w.dtype) for w in weights],
        in_specs=[VMEM] * (1 + n_weights),
        out_specs=[VMEM] * (1 + n_weights),
        scratch_shapes=[pltpu.SemaphoreType.DMA((copies,)), pltpu.SemaphoreType.DMA((copies,))],
        compiler_params=pltpu.CompilerParams(
            collective_id=0, has_side_effects=True, vmem_limit_bytes=48 * 1024 * 1024
        ),
        name="gather_all",
    )(tokens, *weights)


def attention_kernel(n_row, n_col, per_window, heads, band, n_weights, *refs):
    x_ref, qkv_ref, out_w_ref, gain_ref = refs[:4]
    w_in = refs[4 : 4 + n_weights]
    terms = refs[4 + n_weights]
    w_out = refs[5 + n_weights : 5 + 2 * n_weights]
    q_all, kv_all, sem_a, sem_b, kv_send, kv_recv, row_send, row_recv = refs[5 + 2 * n_weights :]
    ring = Ring(n_row, n_col, sem_a, sem_b)
    row, col = ring.row, ring.col
    bands = x_ref.shape[0] // band
    width = heads * HD
    contract = (((1,), (1,)), ((), ()))
    seat = lax.rem(col, per_window)

    def mate(k):
        return (row, col - seat + lax.rem(seat + k, per_window))

    ring.greet([mate(k) for k in range(1, per_window)])
    ring.begin(w_in, w_out)

    def band_rows(b):
        return pl.ds(pl.multiple_of(b * band, band), band)

    def kv_copy(b, k):
        return pltpu.make_async_remote_copy(
            src_ref=kv_all.at[0, :, band_rows(b)],
            dst_ref=kv_all.at[k, :, band_rows(b)],
            send_sem=kv_send.at[b, k],
            recv_sem=kv_recv.at[b, k],
            device_id=mate(k),
            device_id_type=MESH,
        )

    def row_copy(b, r):
        return pltpu.make_async_remote_copy(
            src_ref=terms.at[0, band_rows(b)],
            dst_ref=terms.at[r, band_rows(b)],
            send_sem=row_send.at[b, r],
            recv_sem=row_recv.at[b, r],
            device_id=ring.other_row(r),
            device_id_type=MESH,
        )

    def project(b, carry):
        here = band_rows(b)
        projected = jnp.dot(x_ref[here, :], qkv_ref[...], preferred_element_type=jnp.float32)
        for part in range(2):
            for head in range(heads):
                lo = head * HD
                piece = projected[:, part * width + lo : part * width + lo + HD]
                scaled = (to_sphere(piece) * gain_ref[:, lo : lo + HD]).astype(jnp.bfloat16)
                if part == 0:
                    q_all[here, lo : lo + HD] = scaled
                else:
                    kv_all[0, 0, here, lo : lo + HD] = scaled
        kv_all[0, 1, here, :] = projected[:, 2 * width :].astype(jnp.bfloat16)
        for k in range(1, per_window):
            kv_copy(b, k).start()
        return carry

    lax.fori_loop(0, bands, project, 0)
    for t in range(ring.nz // 2):
        ring.advance(t, w_out)

    def attend(b, carry):
        here = band_rows(b)
        for k in range(1, per_window):
            kv_copy(b, k).wait_recv()
        outs = []
        for head in range(heads):
            cut = slice(head * HD, head * HD + HD)
            query = q_all[here, cut]
            keys = jnp.concatenate([kv_all[k, 0, here, cut] for k in range(per_window)], axis=0)
            values = jnp.concatenate([kv_all[k, 1, here, cut] for k in range(per_window)], axis=0)
            scores = lax.dot_general(query, keys, contract, preferred_element_type=jnp.float32)
            expo = jnp.exp(scores * (1.0 / math.sqrt(HD)))
            weights = (expo / jnp.sum(expo, axis=-1, keepdims=True)).astype(jnp.bfloat16)
            outs.append(
                jnp.dot(weights, values, preferred_element_type=jnp.float32).astype(jnp.bfloat16)
            )
        attended = jnp.concatenate(outs, axis=1)
        terms[0, here, :] = lax.dot_general(
            attended, out_w_ref[...], contract, preferred_element_type=jnp.float32
        ).astype(jnp.bfloat16)
        for r in range(1, n_row):
            row_copy(b, r).start()
        return carry

    lax.fori_loop(0, bands, attend, 0)
    for t in range(ring.nz // 2, ring.nz):
        ring.advance(t, w_out)
    ring.finish()

    def drain(b, carry):
        for k in range(1, per_window):
            kv_copy(b, k).wait_send()
        for r in range(1, n_row):
            row_copy(b, r).wait()
        return carry

    lax.fori_loop(0, bands, drain, 0)


def attention(x, qkv, out_w, gain, weights, n_row, n_col, per_window, band):
    tokens, depth = x.shape
    width = qkv.shape[1] // 3
    heads = width // HD
    bands = tokens // band
    n_weights = len(weights)
    copies = ring_copies(n_col, n_weights)
    dma = pltpu.SemaphoreType.DMA
    return pl.pallas_call(
        functools.partial(attention_kernel, n_row, n_col, per_window, heads, band, n_weights),
        out_shape=[jax.ShapeDtypeStruct((n_row, tokens, depth), jnp.bfloat16)]
        + [jax.ShapeDtypeStruct((n_col,) + w.shape, w.dtype) for w in weights],
        in_specs=[VMEM] * (4 + n_weights),
        out_specs=[VMEM] * (1 + n_weights),
        scratch_shapes=[
            pltpu.VMEM((tokens, width), jnp.bfloat16),
            pltpu.VMEM((per_window, 2, tokens, width), jnp.bfloat16),
            dma((copies,)),
            dma((copies,)),
            dma((bands, per_window)),
            dma((bands, per_window)),
            dma((bands, n_row)),
            dma((bands, n_row)),
        ],
        compiler_params=pltpu.CompilerParams(
            collective_id=1, has_side_effects=True, vmem_limit_bytes=56 * 1024 * 1024
        ),
        name="attention",
    )(x, qkv, out_w, gain.reshape(1, width), *weights)


def on_device(
    tokens,
    shifts,
    qkv_weight,
    out_weight,
    up_weight,
    down_weight,
    qk_gain,
    attn_rate,
    mlp_rate,
    hidden_gain,
):
    n_row = lax.axis_size("row")
    n_col = lax.axis_size("col")
    row = lax.axis_index("row")
    local_rows, cols, width = tokens.shape
    local_width = qkv_weight.shape[2]
    hidden = up_weight.shape[1]
    per_window = WIN // cols
    reach = (WIN + cols - 2) // cols
    strip_rows = local_rows * n_row
    count = strip_rows * cols
    shift_row, shift_col = shifts[0], shifts[1]

    gathered = gather_all(
        tokens.reshape(local_rows * cols, width),
        [qkv_weight.reshape(-1, 3 * local_width), out_weight.T],
        n_row,
        n_col,
        reach,
    )
    pieces = gathered[0].reshape(n_row, reach + 1, local_rows, cols, width)
    qkv_full = gathered[1].reshape(width, 3 * local_width)
    out_full = gathered[2].reshape(width, local_width)

    wide = pieces.transpose(0, 2, 1, 3, 4).reshape(strip_rows, (reach + 1) * cols, width)
    strip = lax.dynamic_slice_in_dim(wide, shift_col, cols, axis=1)
    strip = jnp.roll(strip, -shift_row, axis=0).reshape(count, width)
    flat = to_sphere(strip.astype(jnp.float32))
    second = attention(
        flat.astype(jnp.bfloat16),
        qkv_full,
        out_full,
        qk_gain,
        [up_weight, down_weight.T],
        n_row,
        n_col,
        per_window,
        WIN * cols,
    )
    terms = second[0]
    up_full = second[1].reshape(width, hidden)
    down_full = second[2].reshape(width, hidden)
    attn_all = terms[0].astype(jnp.float32)
    for r in range(1, n_row):
        attn_all = attn_all + terms[r].astype(jnp.float32)
    mixed = to_sphere(flat + attn_rate * (to_sphere(attn_all) - flat))
    raised = jnp.dot(mixed.astype(jnp.bfloat16), up_full, preferred_element_type=jnp.float32)
    activated = jax.nn.gelu(raised * hidden_gain, approximate=False).astype(jnp.bfloat16)
    mlp_own = lax.dot_general(
        activated, down_full, (((1,), (1,)), ((), ())), preferred_element_type=jnp.float32
    ).astype(jnp.bfloat16)

    def part(value, owner):
        lifted = value.reshape(strip_rows, cols, width)
        twice = jnp.concatenate([lifted, lifted], axis=0)
        first = jnp.mod(owner * local_rows - shift_row, strip_rows)
        return lax.dynamic_slice_in_dim(twice, first, local_rows, 0)

    mlp_local = part(mlp_own, row).astype(jnp.float32)
    for r in range(1, n_row):
        there = part(mlp_own, lax.rem(row + r, n_row))
        mlp_local = mlp_local + shifted(there, "row", r).astype(jnp.float32)
    mixed_local = part(mixed, row)
    result = to_sphere(mixed_local + mlp_rate * (to_sphere(mlp_local) - mixed_local))
    result = result.astype(jnp.bfloat16)
    spread = [shifted(result, "col", k) for k in range(reach, 0, -1)] + [result]
    spread = jnp.concatenate(spread, axis=1)
    return lax.dynamic_slice_in_dim(spread, reach * cols - shift_col, cols, axis=1)


def solution(mesh):
    return jax.shard_map(
        on_device,
        mesh=mesh,
        in_specs=(
            P("row", "col", None),
            P(),
            P("col", None, "row"),
            P("row", "col"),
            P("col", "row"),
            P("row", "col"),
            P("row"),
            P(),
            P(),
            P("row"),
        ),
        out_specs=P("row", "col", None),
        check_vma=False,
    )
```

```python
import functools
import math

import jax
import jax.numpy as jnp
from jax import lax
from jax.experimental import pallas as pl
from jax.experimental.pallas import tpu as pltpu
from jax.sharding import PartitionSpec as P

HD = 64
WIN = 16
MESH = pl.DeviceIdType.MESH
VMEM = pl.BlockSpec(memory_space=pltpu.VMEM)


def shifted(value, axis, steps):
    count = lax.axis_size(axis)
    pairs = [(source, (source + steps) % count) for source in range(count)]
    return lax.ppermute(value, axis, pairs)


def to_sphere(vector):
    return vector * lax.rsqrt(jnp.mean(vector * vector, axis=-1, keepdims=True) + 1e-06)


class Ring:
    def __init__(self, n_row, n_col, send_sem, recv_sem):
        self.n_row, self.n_col, self.nz = n_row, n_col, n_col // 4
        self.send_sem, self.recv_sem = send_sem, recv_sem
        self.row, self.col = lax.axis_index("row"), lax.axis_index("col")
        self.z, self.y, self.core = self.col // 4, (self.col // 2) % 2, self.col % 2
        self.z_next = (self.row, self.at(self.z + 1, self.y, self.core))
        self.z_prev = (self.row, self.at(self.z - 1, self.y, self.core))
        self.y_peer = (self.row, self.at(self.z, 1 - self.y, self.core))
        self.core_peer = (self.row, self.at(self.z, self.y, 1 - self.core))
        self.started, self.core_copies, self.z_copy, self.y_copy = [], [], {}, {}

    def at(self, z, y, core):
        return (lax.rem(z + 2 * self.nz, self.nz) * 2 + y) * 2 + core

    def other_row(self, r):
        return (lax.rem(self.row + r, self.n_row), self.col)

    def greet(self, more):
        peers = [self.z_next, self.z_prev, self.y_peer, self.core_peer] + more
        peers += [self.other_row(r) for r in range(1, self.n_row)]
        barrier = pltpu.get_barrier_semaphore()
        for peer in peers:
            pl.semaphore_signal(barrier, inc=1, device_id=peer, device_id_type=MESH)
        pl.semaphore_wait(barrier, len(peers))

    def send(self, src, dst, peer):
        index = len(self.started)
        copy = pltpu.make_async_remote_copy(
            src_ref=src,
            dst_ref=dst,
            send_sem=self.send_sem.at[index],
            recv_sem=self.recv_sem.at[index],
            device_id=peer,
            device_id_type=MESH,
        )
        copy.start()
        self.started.append(copy)
        return copy

    def begin(self, w_in, w_out):
        for w in range(len(w_in)):
            slot = w_out[w].at[self.col]
            self.z_copy[w, 0] = self.send(w_in[w], slot, self.z_next)
            self.y_copy[w, 0] = self.send(w_in[w], slot, self.y_peer)
            self.core_copies.append(self.send(w_in[w], slot, self.core_peer))
        for w in range(len(w_in)):
            w_out[w][self.col] = w_in[w][...]

    def advance(self, t, w_out):
        for w in range(len(w_out)):
            if t > 0:
                self.z_copy[w, t - 1].wait_recv()
                block = w_out[w].at[self.at(self.z - t, self.y, self.core)]
                if t < self.nz - 1:
                    self.z_copy[w, t] = self.send(block, block, self.z_next)
                self.y_copy[w, t] = self.send(block, block, self.y_peer)
                self.core_copies.append(self.send(block, block, self.core_peer))
        last = t == self.nz - 1
        for late in ([t - 1] if t > 0 else []) + ([t] if last else []):
            for w in range(len(w_out)):
                self.y_copy[w, late].wait_recv()
                other = w_out[w].at[self.at(self.z - late, 1 - self.y, self.core)]
                self.core_copies.append(self.send(other, other, self.core_peer))

    def finish(self):
        for copy in self.core_copies:
            copy.wait_recv()
        for copy in self.started:
            copy.wait_send()


def gather_kernel(n_row, n_col, reach, n_weights, *refs):
    tok_in = refs[0]
    w_in = refs[1 : 1 + n_weights]
    tok_out = refs[1 + n_weights]
    w_out = refs[2 + n_weights : 2 + 2 * n_weights]
    ring = Ring(n_row, n_col, *refs[2 + 2 * n_weights :])
    row, col = ring.row, ring.col
    ring.greet(
        [(row, lax.rem(col + k, n_col)) for k in range(1, reach + 1)]
        + [(row, lax.rem(col - k + n_col, n_col)) for k in range(1, reach + 1)]
    )
    near = {}
    far = []
    for k in range(1, reach + 1):
        near[k] = ring.send(tok_in, tok_out.at[row, k], (row, lax.rem(col - k + n_col, n_col)))
    for r in range(1, n_row):
        far.append(ring.send(tok_in, tok_out.at[row, 0], ring.other_row(r)))
    ring.begin(w_in, w_out)
    tok_out[row, 0] = tok_in[...]
    for t in range(ring.nz):
        if t == 1:
            for k in range(1, reach + 1):
                near[k].wait_recv()
                piece = tok_out.at[row, k]
                for r in range(1, n_row):
                    far.append(ring.send(piece, piece, ring.other_row(r)))
        ring.advance(t, w_out)
    for copy in far:
        copy.wait_recv()
    ring.finish()


def ring_copies(n_col, n_weights):
    nz = n_col // 4
    return n_weights * (nz - 1 + nz + 2 * nz)


def gather_all(tokens, weights, n_row, n_col, reach):
    n_weights = len(weights)
    copies = reach * n_row + (n_row - 1) + ring_copies(n_col, n_weights)
    return pl.pallas_call(
        functools.partial(gather_kernel, n_row, n_col, reach, n_weights),
        out_shape=[jax.ShapeDtypeStruct((n_row, reach + 1) + tokens.shape, tokens.dtype)]
        + [jax.ShapeDtypeStruct((n_col,) + w.shape, w.dtype) for w in weights],
        in_specs=[VMEM] * (1 + n_weights),
        out_specs=[VMEM] * (1 + n_weights),
        scratch_shapes=[pltpu.SemaphoreType.DMA((copies,)), pltpu.SemaphoreType.DMA((copies,))],
        compiler_params=pltpu.CompilerParams(
            collective_id=0, has_side_effects=True, vmem_limit_bytes=48 * 1024 * 1024
        ),
        name="gather_all",
    )(tokens, *weights)


def attention_kernel(n_row, n_col, per_window, heads, band, n_weights, *refs):
    x_ref, qkv_ref, out_w_ref, gain_ref = refs[:4]
    w_in = refs[4 : 4 + n_weights]
    terms = refs[4 + n_weights]
    w_out = refs[5 + n_weights : 5 + 2 * n_weights]
    q_all, kv_all, sem_a, sem_b, kv_send, kv_recv, row_send, row_recv = refs[5 + 2 * n_weights :]
    ring = Ring(n_row, n_col, sem_a, sem_b)
    row, col = ring.row, ring.col
    bands = x_ref.shape[0] // band
    width = heads * HD
    contract = (((1,), (1,)), ((), ()))
    seat = lax.rem(col, per_window)

    def mate(k):
        return (row, col - seat + lax.rem(seat + k, per_window))

    ring.greet([mate(k) for k in range(1, per_window)])
    ring.begin(w_in, w_out)

    def band_rows(b):
        return pl.ds(pl.multiple_of(b * band, band), band)

    def kv_copy(b, k):
        return pltpu.make_async_remote_copy(
            src_ref=kv_all.at[0, :, band_rows(b)],
            dst_ref=kv_all.at[k, :, band_rows(b)],
            send_sem=kv_send.at[b, k],
            recv_sem=kv_recv.at[b, k],
            device_id=mate(k),
            device_id_type=MESH,
        )

    def row_copy(b, r):
        return pltpu.make_async_remote_copy(
            src_ref=terms.at[0, band_rows(b)],
            dst_ref=terms.at[r, band_rows(b)],
            send_sem=row_send.at[b, r],
            recv_sem=row_recv.at[b, r],
            device_id=ring.other_row(r),
            device_id_type=MESH,
        )

    def project(b, carry):
        here = band_rows(b)
        projected = jnp.dot(x_ref[here, :], qkv_ref[...], preferred_element_type=jnp.float32)
        for part in range(2):
            for head in range(heads):
                lo = head * HD
                piece = projected[:, part * width + lo : part * width + lo + HD]
                scaled = (to_sphere(piece) * gain_ref[:, lo : lo + HD]).astype(jnp.bfloat16)
                if part == 0:
                    q_all[here, lo : lo + HD] = scaled
                else:
                    kv_all[0, 0, here, lo : lo + HD] = scaled
        kv_all[0, 1, here, :] = projected[:, 2 * width :].astype(jnp.bfloat16)
        for k in range(1, per_window):
            kv_copy(b, k).start()
        return carry

    lax.fori_loop(0, bands, project, 0)
    for t in range(ring.nz // 2):
        ring.advance(t, w_out)

    def attend(b, carry):
        here = band_rows(b)
        for k in range(1, per_window):
            kv_copy(b, k).wait_recv()
        outs = []
        for head in range(heads):
            cut = slice(head * HD, head * HD + HD)
            query = q_all[here, cut]
            keys = jnp.concatenate([kv_all[k, 0, here, cut] for k in range(per_window)], axis=0)
            values = jnp.concatenate([kv_all[k, 1, here, cut] for k in range(per_window)], axis=0)
            scores = lax.dot_general(query, keys, contract, preferred_element_type=jnp.float32)
            expo = jnp.exp(scores * (1.0 / math.sqrt(HD)))
            weights = (expo / jnp.sum(expo, axis=-1, keepdims=True)).astype(jnp.bfloat16)
            outs.append(
                jnp.dot(weights, values, preferred_element_type=jnp.float32).astype(jnp.bfloat16)
            )
        attended = jnp.concatenate(outs, axis=1)
        terms[0, here, :] = lax.dot_general(
            attended, out_w_ref[...], contract, preferred_element_type=jnp.float32
        ).astype(jnp.bfloat16)
        for r in range(1, n_row):
            row_copy(b, r).start()
        return carry

    lax.fori_loop(0, bands, attend, 0)
    for t in range(ring.nz // 2, ring.nz):
        ring.advance(t, w_out)
    ring.finish()

    def drain(b, carry):
        for k in range(1, per_window):
            kv_copy(b, k).wait_send()
        for r in range(1, n_row):
            row_copy(b, r).wait()
        return carry

    lax.fori_loop(0, bands, drain, 0)


def attention(x, qkv, out_w, gain, weights, n_row, n_col, per_window, band):
    tokens, depth = x.shape
    width = qkv.shape[1] // 3
    heads = width // HD
    bands = tokens // band
    n_weights = len(weights)
    copies = ring_copies(n_col, n_weights)
    dma = pltpu.SemaphoreType.DMA
    return pl.pallas_call(
        functools.partial(attention_kernel, n_row, n_col, per_window, heads, band, n_weights),
        out_shape=[jax.ShapeDtypeStruct((n_row, tokens, depth), jnp.bfloat16)]
        + [jax.ShapeDtypeStruct((n_col,) + w.shape, w.dtype) for w in weights],
        in_specs=[VMEM] * (4 + n_weights),
        out_specs=[VMEM] * (1 + n_weights),
        scratch_shapes=[
            pltpu.VMEM((tokens, width), jnp.bfloat16),
            pltpu.VMEM((per_window, 2, tokens, width), jnp.bfloat16),
            dma((copies,)),
            dma((copies,)),
            dma((bands, per_window)),
            dma((bands, per_window)),
            dma((bands, n_row)),
            dma((bands, n_row)),
        ],
        compiler_params=pltpu.CompilerParams(
            collective_id=1, has_side_effects=True, vmem_limit_bytes=56 * 1024 * 1024
        ),
        name="attention",
    )(x, qkv, out_w, gain.reshape(1, width), *weights)


def on_device(
    tokens,
    shifts,
    qkv_weight,
    out_weight,
    up_weight,
    down_weight,
    qk_gain,
    attn_rate,
    mlp_rate,
    hidden_gain,
):
    n_row = lax.axis_size("row")
    n_col = lax.axis_size("col")
    row = lax.axis_index("row")
    local_rows, cols, width = tokens.shape
    local_width = qkv_weight.shape[2]
    hidden = up_weight.shape[1]
    per_window = WIN // cols
    reach = (WIN + cols - 2) // cols
    strip_rows = local_rows * n_row
    count = strip_rows * cols
    shift_row, shift_col = shifts[0], shifts[1]

    gathered = gather_all(
        tokens.reshape(local_rows * cols, width),
        [qkv_weight.reshape(-1, 3 * local_width), out_weight.T],
        n_row,
        n_col,
        reach,
    )
    pieces = gathered[0].reshape(n_row, reach + 1, local_rows, cols, width)
    qkv_full = gathered[1].reshape(width, 3 * local_width)
    out_full = gathered[2].reshape(width, local_width)

    wide = pieces.transpose(0, 2, 1, 3, 4).reshape(strip_rows, (reach + 1) * cols, width)
    strip = lax.dynamic_slice_in_dim(wide, shift_col, cols, axis=1)
    strip = jnp.roll(strip, -shift_row, axis=0).reshape(count, width)
    flat = to_sphere(strip.astype(jnp.float32))
    second = attention(
        flat.astype(jnp.bfloat16),
        qkv_full,
        out_full,
        qk_gain,
        [up_weight, down_weight.T],
        n_row,
        n_col,
        per_window,
        WIN * cols,
    )
    terms = second[0]
    up_full = second[1].reshape(width, hidden)
    down_full = second[2].reshape(width, hidden)
    attn_all = terms[0].astype(jnp.float32)
    for r in range(1, n_row):
        attn_all = attn_all + terms[r].astype(jnp.float32)
    mixed = to_sphere(flat + attn_rate * (to_sphere(attn_all) - flat))

    def feed_forward(rows):
        raised = jnp.dot(rows, up_full, preferred_element_type=jnp.float32)
        activated = jax.nn.gelu(raised * hidden_gain, approximate=False).astype(jnp.bfloat16)
        return lax.dot_general(
            activated, down_full, (((1,), (1,)), ((), ())), preferred_element_type=jnp.float32
        ).astype(jnp.bfloat16)

    def part(value, owner):
        lifted = value.reshape(strip_rows, cols, width)
        twice = jnp.concatenate([lifted, lifted], axis=0)
        first = jnp.mod(owner * local_rows - shift_row, strip_rows)
        return lax.dynamic_slice_in_dim(twice, first, local_rows, 0)

    mixed_bf = mixed.astype(jnp.bfloat16)
    own = part(mixed_bf, row).reshape(local_rows * cols, width)
    moved = []
    for r in range(1, n_row):
        there = feed_forward(part(mixed_bf, lax.rem(row + r, n_row)).reshape(own.shape))
        own, there = lax.optimization_barrier((own, there))
        moved.append(shifted(there, "row", r))
    mlp_local = feed_forward(own).astype(jnp.float32)
    for arrived in moved:
        mlp_local = mlp_local + arrived.astype(jnp.float32)
    mlp_local = mlp_local.reshape(local_rows, cols, width)
    mixed_local = part(mixed, row)
    result = to_sphere(mixed_local + mlp_rate * (to_sphere(mlp_local) - mixed_local))
    result = result.astype(jnp.bfloat16)
    spread = [shifted(result, "col", k) for k in range(reach, 0, -1)] + [result]
    spread = jnp.concatenate(spread, axis=1)
    return lax.dynamic_slice_in_dim(spread, reach * cols - shift_col, cols, axis=1)


def solution(mesh):
    return jax.shard_map(
        on_device,
        mesh=mesh,
        in_specs=(
            P("row", "col", None),
            P(),
            P("col", None, "row"),
            P("row", "col"),
            P("col", "row"),
            P("row", "col"),
            P("row"),
            P(),
            P(),
            P("row"),
        ),
        out_specs=P("row", "col", None),
        check_vma=False,
    )
```
